128 devices in a mesh: hi: 8 (over z_hi, y), lo: 16 (over z_lo, x, core).
Axes of the slice: x: 4, y: 4, z: 4 (z_hi: 2, z_lo: 2; z = z_hi * 2 + z_lo), core: 2. Of those that a mesh axis runs over, the one named last changes fastest.
Arguments:
- charges: bfloat16 [1048576, 128], P(('hi', 'lo')), may hold values from -6 to 6
- source_order: int32 [1048576], P(('hi', 'lo')), may hold values from 0 to 8191, as said below
- source_interp: bfloat16 [1048576, 128], P(('hi', 'lo')), may hold values from -0.5 to 0.5
- factors: bfloat16 [16384, 8, 128], P(('hi', 'lo')), may hold values from -6 to 6
- transfers: bfloat16 [8, 2, 2, 64, 128], replicated, may hold values from -0.375 to 0.375
- level_bits: int32 [4], replicated, may hold values from 0 to 6
- receiver_interp: bfloat16 [1048576, 128], P(('hi', 'lo')), may hold values from -0.5 to 0.5
- receiver_slot: int32 [1048576], P(('hi', 'lo')), may hold values from 0 to 8191, as said below
Outputs:
- displacement: bfloat16 [1048576, 128], P(('hi', 'lo'))
The draws below stay inside these ranges and needn't reach their ends.
Inputs may be any that keep to these rules, and one draw needn't show every extreme that they name: `source_order`: each aligned block of 8192 entries is a permutation of 0 to 8191. `receiver_slot`: each aligned block of 8192 entries is a permutation of 0 to 8191.
All inputs are finite; a program needn't handle non-finite values.
Results may differ from the reference program's by a relative error of at most 0.019.
Values may be sent and summed in bfloat16 or wider, within the bound.
A program may use at most 64 MiB of HBM per device.

```python
import jax
import jax.numpy as jnp
from jax import lax

RANK = 64
RHS = 64
LEAF = 64
BLK_DEV = 128
BLOCKS = 16384
PTS_DEV = 8192
POINTS = 1048576
N_LO = 16
DEVICES = 128


def block_permutations(key):
    keys = jax.random.split(key, POINTS // PTS_DEV)
    perms = jax.vmap(lambda single: jax.random.permutation(single, PTS_DEV))(keys)
    return perms.reshape(-1).astype(jnp.int32)


def draw_source_order(key, part):
    return block_permutations(jax.random.fold_in(key, 11))


def draw_receiver_slot(key, part):
    return block_permutations(jax.random.fold_in(key, 29))


def place_ends(array, own_key, least, largest):
    longest = array.shape.index(max(array.shape))
    spots = []
    for shift in (0, 1):
        where = [jax.random.randint(jax.random.fold_in(own_key, axis), (), 0, length) for axis, length in enumerate(array.shape)]
        where[longest] = (where[longest] + shift) % array.shape[longest]
        spots.append(tuple(where))
    return array.at[spots[0]].set(least).at[spots[1]].set(largest)


def steps_of(key, dims, shards, least, top_value):
    loudness = 1.0
    for dim, parts in shards:
        steps = jax.random.uniform(jax.random.fold_in(jax.random.fold_in(key, 6), dim), (parts,), jnp.float32, least / len(shards), top_value / len(shards))
        loudness = loudness * jnp.repeat(jnp.exp(steps), dims[dim] // parts).reshape((-1,) + (1,) * (len(dims) - 1 - dim))
    return loudness


def bell_draw(rng, dims, scale, reach, cuts=(), held_as=jnp.bfloat16):
    entries = scale * jax.random.normal(rng, dims, jnp.float32)
    if cuts:
        entries = entries * steps_of(rng, dims, cuts, -0.22, 0.18)
    return jnp.clip(entries, -reach, reach).astype(held_as)


def setup_inputs(seed: int = 0) -> dict:
    splits = jax.random.split(jax.random.key(seed), 9)
    return {
        "charges": bell_draw(splits[0], (POINTS, 2 * RHS), 0.7071, 6.0, ((0, 128),)),
        "source_order": draw_source_order(jax.random.fold_in(splits[8], 71), 0),
        "source_interp": bell_draw(splits[2], (POINTS, 2 * RANK), (2 * LEAF) ** -0.5, 0.5, ((0, 128),)),
        "factors": bell_draw(splits[3], (BLOCKS, 8, 2 * RANK), 0.7071, 6.0, ((0, 128),)),
        "transfers": bell_draw(splits[4], (8, 2, 2, RANK, 2 * RANK), (4 * RANK) ** -0.5, 0.375),
        "level_bits": place_ends(jax.random.randint(splits[5], (4,), 0, 7), jax.random.fold_in(splits[5], 1), 0, 6).astype(jnp.int32),
        "receiver_interp": bell_draw(splits[6], (POINTS, 2 * RANK), (2 * RANK) ** -0.5, 0.5, ((0, 128),)),
        "receiver_slot": draw_receiver_slot(jax.random.fold_in(splits[8], 71), 0),
    }


def real_form(block_piece):
    rank_size = block_piece.shape[0]
    real_part = block_piece[:, :rank_size]
    imag_part = block_piece[:, rank_size:]
    lower_rows = jnp.concatenate([-imag_part, real_part], axis=1)
    return jnp.concatenate([block_piece, lower_rows], axis=0)


def times_factor(values, factor):
    rank_size = factor.shape[-1] // 2
    widened = factor.astype(jnp.float32)[:, None, :]
    factor_re = widened[..., :rank_size]
    factor_im = widened[..., rank_size:]
    values_re = values[..., :rank_size]
    values_im = values[..., rank_size:]
    return jnp.concatenate([values_re * factor_re - values_im * factor_im, values_re * factor_im + values_im * factor_re], axis=-1)


def apply_matrix(coeffs, matrix):
    pair_width = coeffs.shape[-1]
    flattened = coeffs.reshape(-1, pair_width)
    return jnp.dot(flattened, real_form(matrix), preferred_element_type=jnp.float32).reshape(coeffs.shape)


def mix_halves(lower_half, upper_half, matrices):
    child_zero = apply_matrix(lower_half, matrices[0, 0]) + apply_matrix(upper_half, matrices[0, 1])
    child_one = apply_matrix(lower_half, matrices[1, 0]) + apply_matrix(upper_half, matrices[1, 1])
    return child_zero, child_one


def pair_level(coeffs, factor, matrices, stride):
    blocks_here = coeffs.shape[0]
    half_index = jnp.arange(blocks_here // 2, dtype=jnp.int32)
    lower_index = (half_index // stride) * (2 * stride) + half_index % stride
    upper_index = lower_index + stride
    child_zero, child_one = mix_halves(coeffs[lower_index], coeffs[upper_index], matrices)
    blocks = jnp.arange(blocks_here, dtype=jnp.int32)
    child_bit = (blocks // stride) % 2
    position = child_bit * (blocks_here // 2) + (blocks // (2 * stride)) * stride + blocks % stride
    merged = jnp.concatenate([child_zero, child_one], axis=0)[position]
    return times_factor(merged, factor).astype(jnp.bfloat16)


def leaf_coeffs(pair_rows):
    charge_rows, interp_rows = pair_rows
    rhs_count = charge_rows.shape[-1] // 2
    rank_size = interp_rows.shape[-1] // 2
    products = jnp.einsum("bmk,bmr->bkr", charge_rows.astype(jnp.float32), interp_rows.astype(jnp.float32))
    real_part = products[:, :rhs_count, :rank_size] - products[:, rhs_count:, rank_size:]
    imag_part = products[:, :rhs_count, rank_size:] + products[:, rhs_count:, :rank_size]
    return jnp.concatenate([real_part, imag_part], axis=-1).astype(jnp.bfloat16)


def receiver_values(pair_rows):
    interp_rows, final_rows = pair_rows
    rank_size = interp_rows.shape[-1] // 2
    coeff_re = final_rows[..., :rank_size]
    coeff_im = final_rows[..., rank_size:]
    stacked = jnp.concatenate([jnp.concatenate([coeff_re, -coeff_im], axis=-1), jnp.concatenate([coeff_im, coeff_re], axis=-1)], axis=1)
    values = jnp.einsum("bmr,bnr->bmn", interp_rows.astype(jnp.float32), stacked.astype(jnp.float32))
    return values.astype(jnp.bfloat16)


def reference(charges, source_order, source_interp, factors, transfers, level_bits, receiver_interp, receiver_slot):
    device_rows = (jnp.arange(POINTS, dtype=jnp.int32) // PTS_DEV) * PTS_DEV
    ordered = charges[device_rows + source_order]
    coeffs = lax.map(leaf_coeffs, (ordered.reshape(DEVICES, BLK_DEV, LEAF, 2 * RHS), source_interp.reshape(DEVICES, BLK_DEV, LEAF, 2 * RANK)))
    coeffs = coeffs.reshape(BLOCKS, RHS, 2 * RANK)
    strides = jnp.left_shift(jnp.int32(1), level_bits)
    coeffs = pair_level(coeffs, factors[:, 0], transfers[0], strides[0])
    coeffs = pair_level(coeffs, factors[:, 1], transfers[1], strides[1])
    coeffs = pair_level(coeffs, factors[:, 2], transfers[2], BLK_DEV * N_LO // 2)
    coeffs = pair_level(coeffs, factors[:, 3], transfers[3], BLOCKS // 2)
    share_size = BLK_DEV // DEVICES
    switched = coeffs.reshape(DEVICES, DEVICES, share_size, RHS, 2 * RANK).transpose(1, 0, 2, 3, 4).reshape(BLOCKS, RHS, 2 * RANK)
    moved_factors = factors[:, 4:].reshape(DEVICES, DEVICES, share_size, 4, 2 * RANK).transpose(1, 0, 2, 3, 4).reshape(BLOCKS, 4, 2 * RANK)
    coeffs = pair_level(switched, moved_factors[:, 0], transfers[4], strides[2])
    coeffs = pair_level(coeffs, moved_factors[:, 1], transfers[5], strides[3])
    coeffs = pair_level(coeffs, moved_factors[:, 2], transfers[6], BLK_DEV * N_LO // 2)
    coeffs = pair_level(coeffs, moved_factors[:, 3], transfers[7], BLOCKS // 2)
    tree_values = lax.map(receiver_values, (receiver_interp.reshape(DEVICES, BLK_DEV, LEAF, 2 * RANK), coeffs.reshape(DEVICES, BLK_DEV, RHS, 2 * RANK)))
    tree_values = tree_values.reshape(POINTS, 2 * RHS)
    return tree_values[device_rows + receiver_slot]
```

```python
import jax
import jax.numpy as jnp
from jax import lax
from jax.sharding import PartitionSpec as P

LEAF = 64


def partner_2(value, axis, bit):
    mask = 2**bit
    pairs = [(source, source ^ mask) for source in range(lax.axis_size(axis))]
    return lax.ppermute(value, axis, pairs)


def real_form(block_piece):
    rank_size = block_piece.shape[0]
    real_part = block_piece[:, :rank_size]
    imag_part = block_piece[:, rank_size:]
    lower_rows = jnp.concatenate([-imag_part, real_part], axis=1)
    return jnp.concatenate([block_piece, lower_rows], axis=0)


def times_factor(values, factor):
    rank_size = factor.shape[-1] // 2
    widened = factor.astype(jnp.float32)[:, None, :]
    factor_re = widened[..., :rank_size]
    factor_im = widened[..., rank_size:]
    values_re = values[..., :rank_size]
    values_im = values[..., rank_size:]
    return jnp.concatenate(
        [
            values_re * factor_re - values_im * factor_im,
            values_re * factor_im + values_im * factor_re,
        ],
        axis=-1,
    )


def apply_matrix(coeffs, matrix):
    pair_width = coeffs.shape[-1]
    flattened = coeffs.reshape(-1, pair_width)
    return jnp.dot(flattened, real_form(matrix), preferred_element_type=jnp.float32).reshape(
        coeffs.shape
    )


def mix_halves(lower_half, upper_half, matrices):
    child_zero = apply_matrix(lower_half, matrices[0, 0]) + apply_matrix(upper_half, matrices[0, 1])
    child_one = apply_matrix(lower_half, matrices[1, 0]) + apply_matrix(upper_half, matrices[1, 1])
    return (child_zero, child_one)


def local_level(coeffs, factor, matrices, stride):
    blocks_here = coeffs.shape[0]
    half_index = jnp.arange(blocks_here // 2, dtype=jnp.int32)
    lower_index = half_index // stride * (2 * stride) + half_index % stride
    upper_index = lower_index + stride
    child_zero, child_one = mix_halves(coeffs[lower_index], coeffs[upper_index], matrices)
    blocks = jnp.arange(blocks_here, dtype=jnp.int32)
    child_bit = blocks // stride % 2
    position = child_bit * (blocks_here // 2) + blocks // (2 * stride) * stride + blocks % stride
    merged = jnp.concatenate([child_zero, child_one], axis=0)[position]
    return times_factor(merged, factor).astype(jnp.bfloat16)


def static_level(coeffs, factor, matrices, stride):
    blocks_here, rows, width = coeffs.shape
    grouped = coeffs.reshape(blocks_here // (2 * stride), 2, stride, rows, width)
    child_zero, child_one = mix_halves(grouped[:, 0], grouped[:, 1], matrices)
    merged = jnp.stack([child_zero, child_one], axis=1).reshape(coeffs.shape)
    return times_factor(merged, factor).astype(jnp.bfloat16)


def remote_level(coeffs, partner, factor, matrices, own_child):
    own_row = lax.dynamic_index_in_dim(matrices, own_child, 0, keepdims=False)
    own_matrix = lax.dynamic_index_in_dim(own_row, own_child, 0, keepdims=False)
    other_matrix = lax.dynamic_index_in_dim(own_row, 1 - own_child, 0, keepdims=False)
    summed = apply_matrix(coeffs, own_matrix) + apply_matrix(partner, other_matrix)
    return times_factor(summed, factor).astype(jnp.bfloat16)


def per_device(
    charges,
    source_order,
    source_interp,
    factors,
    transfers,
    level_bits,
    receiver_interp,
    receiver_slot,
):
    points, twice_rhs = charges.shape
    rhs_count = twice_rhs // 2
    pair_width = source_interp.shape[1]
    rank_size = pair_width // 2
    blocks_here = points // LEAF
    ordered = charges[source_order].reshape(blocks_here, LEAF, twice_rhs)
    products = jnp.einsum(
        "bmk,bmr->bkr",
        ordered,
        source_interp.reshape(blocks_here, LEAF, pair_width),
        preferred_element_type=jnp.float32,
    )
    real_part = products[:, :rhs_count, :rank_size] - products[:, rhs_count:, rank_size:]
    imag_part = products[:, :rhs_count, rank_size:] + products[:, rhs_count:, :rank_size]
    coeffs = jnp.concatenate([real_part, imag_part], axis=-1).astype(jnp.bfloat16)
    strides = jnp.left_shift(jnp.int32(1), level_bits)
    coeffs = local_level(coeffs, factors[:, 0], transfers[0], strides[0])
    coeffs = local_level(coeffs, factors[:, 1], transfers[1], strides[1])
    inner_bit = lax.axis_size("lo").bit_length() - 2
    outer_bit = lax.axis_size("hi").bit_length() - 2
    inner_child = lax.axis_index("lo") >> inner_bit & 1
    outer_child = lax.axis_index("hi") >> outer_bit & 1
    carried = factors[:, 2:]
    coeffs, carried = (
        lax.all_to_all(coeffs, ("hi", "lo"), split_axis=0, concat_axis=0, tiled=True),
        lax.all_to_all(carried, ("hi", "lo"), split_axis=0, concat_axis=0, tiled=True),
    )
    lo_stride = 2**inner_bit
    hi_stride = lax.axis_size("lo") * 2**outer_bit
    coeffs = static_level(coeffs, carried[:, 0], transfers[2], lo_stride)
    coeffs = static_level(coeffs, carried[:, 1], transfers[3], hi_stride)
    coeffs = local_level(coeffs, carried[:, 2], transfers[4], strides[2])
    coeffs = local_level(coeffs, carried[:, 3], transfers[5], strides[3])
    partner = partner_2(coeffs, "lo", inner_bit)
    coeffs = remote_level(coeffs, partner, carried[:, 4], transfers[6], inner_child)
    partner = partner_2(coeffs, "hi", outer_bit)
    coeffs = remote_level(coeffs, partner, carried[:, 5], transfers[7], outer_child)
    coeff_re = coeffs[..., :rank_size]
    coeff_im = coeffs[..., rank_size:]
    stacked = jnp.concatenate(
        [
            jnp.concatenate([coeff_re, -coeff_im], axis=-1),
            jnp.concatenate([coeff_im, coeff_re], axis=-1),
        ],
        axis=1,
    )
    values = jnp.einsum(
        "bmr,bnr->bmn",
        receiver_interp.reshape(blocks_here, LEAF, pair_width),
        stacked,
        preferred_element_type=jnp.float32,
    )
    tree_values = values.astype(jnp.bfloat16).reshape(points, twice_rhs)
    return tree_values[receiver_slot]


def solution(mesh):
    return jax.shard_map(
        per_device,
        mesh=mesh,
        in_specs=(
            P(("hi", "lo"), None),
            P(("hi", "lo")),
            P(("hi", "lo"), None),
            P(("hi", "lo"), None, None),
            P(),
            P(),
            P(("hi", "lo"), None),
            P(("hi", "lo")),
        ),
        out_specs=P(("hi", "lo"), None),
        check_vma=False,
    )
```

```python
import jax
import jax.numpy as jnp
from jax import lax
from jax.experimental import pallas as pl
from jax.experimental.pallas import tpu as pltpu
from jax.sharding import PartitionSpec as P

LEAF = 64
PAIRS_PER_DOT = 8


def pair_weights(matrices):
    def rf(m):
        r, i = m[:, :64], m[:, 64:]
        return jnp.concatenate([m, jnp.concatenate([-i, r], axis=1)], axis=0)
    top = jnp.concatenate([rf(matrices[0, 0]), rf(matrices[1, 0])], axis=1)
    bottom = jnp.concatenate([rf(matrices[0, 1]), rf(matrices[1, 1])], axis=1)
    return jnp.concatenate([top, bottom], axis=0)


def factor_pair(factor):
    wide = factor.astype(jnp.float32)
    re, im = wide[:, :64], wide[:, 64:]
    return (jnp.concatenate([re, re], axis=1)[:, None, :],
            jnp.concatenate([-im, im], axis=1)[:, None, :])


def levels_kernel(bits_ref, x_ref, w_ref, a_ref, b_ref, o_ref, buf, lhs):
    count = w_ref.shape[0]
    blocks, rows, width = x_ref.shape
    chunks = blocks // 2 // PAIRS_PER_DOT
    for level in range(count):
        src = x_ref if level == 0 else buf.at[(level - 1) % 2]
        dst = o_ref if level == count - 1 else buf.at[level % 2]
        bit = bits_ref[level]
        stride = jnp.left_shift(jnp.int32(1), bit)

        def pair_of(p):
            low = jnp.left_shift(jnp.right_shift(p, bit), bit + 1) + jnp.bitwise_and(p, stride - 1)
            return low, low + stride

        def chunk(g, carry):
            for j in range(PAIRS_PER_DOT):
                n0, n1 = pair_of(g * PAIRS_PER_DOT + j)
                lhs[j * rows:(j + 1) * rows, 0:width] = src[n0]
                lhs[j * rows:(j + 1) * rows, width:2 * width] = src[n1]
            y = jnp.dot(lhs[...], w_ref[level], preferred_element_type=jnp.float32)
            for j in range(PAIRS_PER_DOT):
                n0, n1 = pair_of(g * PAIRS_PER_DOT + j)
                for half, n in ((0, n0), (1, n1)):
                    part = y[j * rows:(j + 1) * rows, half * width:(half + 1) * width]
                    turned = pltpu.roll(part, width // 2, 1)
                    dst[n] = (part * a_ref[level, n] + turned * b_ref[level, n]).astype(dst.dtype)
            return carry

        lax.fori_loop(0, chunks, chunk, 0)


def run_levels(coeffs, bits, matrices_list, factor_list):
    count = len(matrices_list)
    weights = jnp.stack([pair_weights(m) for m in matrices_list])
    pairs = [factor_pair(f) for f in factor_list]
    a = jnp.stack([p[0] for p in pairs])
    b = jnp.stack([p[1] for p in pairs])
    blocks, rows, width = coeffs.shape
    vmem = pl.BlockSpec(memory_space=pltpu.VMEM)
    return pl.pallas_call(
        levels_kernel,
        out_shape=jax.ShapeDtypeStruct(coeffs.shape, jnp.bfloat16),
        in_specs=[pl.BlockSpec(memory_space=pltpu.SMEM)] + [vmem] * 4,
        out_specs=vmem,
        scratch_shapes=[
            pltpu.VMEM((2, blocks, rows, width), jnp.bfloat16),
            pltpu.VMEM((PAIRS_PER_DOT * rows, 2 * width), jnp.bfloat16),
        ],
        cost_estimate=pl.CostEstimate(
            flops=count * blocks * rows * 2 * width * 2 * width,
            bytes_accessed=2 * coeffs.size * 2, transcendentals=0),
    )(bits, coeffs, weights, a, b)


def partner_2(value, axis, bit):
    mask = 2**bit
    pairs = [(source, source ^ mask) for source in range(lax.axis_size(axis))]
    return lax.ppermute(value, axis, pairs)


def real_form(block_piece):
    rank_size = block_piece.shape[0]
    real_part = block_piece[:, :rank_size]
    imag_part = block_piece[:, rank_size:]
    lower_rows = jnp.concatenate([-imag_part, real_part], axis=1)
    return jnp.concatenate([block_piece, lower_rows], axis=0)


def times_factor(values, factor):
    rank_size = factor.shape[-1] // 2
    widened = factor.astype(jnp.float32)[:, None, :]
    factor_re = widened[..., :rank_size]
    factor_im = widened[..., rank_size:]
    values_re = values[..., :rank_size]
    values_im = values[..., rank_size:]
    return jnp.concatenate(
        [
            values_re * factor_re - values_im * factor_im,
            values_re * factor_im + values_im * factor_re,
        ],
        axis=-1,
    )


def apply_matrix(coeffs, matrix):
    pair_width = coeffs.shape[-1]
    flattened = coeffs.reshape(-1, pair_width)
    return jnp.dot(flattened, real_form(matrix), preferred_element_type=jnp.float32).reshape(
        coeffs.shape
    )


def mix_halves(lower_half, upper_half, matrices):
    child_zero = apply_matrix(lower_half, matrices[0, 0]) + apply_matrix(upper_half, matrices[0, 1])
    child_one = apply_matrix(lower_half, matrices[1, 0]) + apply_matrix(upper_half, matrices[1, 1])
    return (child_zero, child_one)


def remote_level(coeffs, partner, factor, matrices, own_child):
    own_row = lax.dynamic_index_in_dim(matrices, own_child, 0, keepdims=False)
    own_matrix = lax.dynamic_index_in_dim(own_row, own_child, 0, keepdims=False)
    other_matrix = lax.dynamic_index_in_dim(own_row, 1 - own_child, 0, keepdims=False)
    summed = apply_matrix(coeffs, own_matrix) + apply_matrix(partner, other_matrix)
    return times_factor(summed, factor).astype(jnp.bfloat16)


def per_device(
    charges,
    source_order,
    source_interp,
    factors,
    transfers,
    level_bits,
    receiver_interp,
    receiver_slot,
):
    points, twice_rhs = charges.shape
    rhs_count = twice_rhs // 2
    pair_width = source_interp.shape[1]
    rank_size = pair_width // 2
    blocks_here = points // LEAF
    ordered = charges[source_order].reshape(blocks_here, LEAF, twice_rhs)
    products = jnp.einsum(
        "bmk,bmr->bkr",
        ordered,
        source_interp.reshape(blocks_here, LEAF, pair_width),
        preferred_element_type=jnp.float32,
    )
    real_part = products[:, :rhs_count, :rank_size] - products[:, rhs_count:, rank_size:]
    imag_part = products[:, :rhs_count, rank_size:] + products[:, rhs_count:, :rank_size]
    coeffs = jnp.concatenate([real_part, imag_part], axis=-1).astype(jnp.bfloat16)
    coeffs = run_levels(
        coeffs, level_bits[:2], [transfers[0], transfers[1]], [factors[:, 0], factors[:, 1]]
    )
    inner_bit = lax.axis_size("lo").bit_length() - 2
    outer_bit = lax.axis_size("hi").bit_length() - 2
    inner_child = lax.axis_index("lo") >> inner_bit & 1
    outer_child = lax.axis_index("hi") >> outer_bit & 1
    carried = factors[:, 2:]
    coeffs, carried = (
        lax.all_to_all(coeffs, ("hi", "lo"), split_axis=0, concat_axis=0, tiled=True),
        lax.all_to_all(carried, ("hi", "lo"), split_axis=0, concat_axis=0, tiled=True),
    )
    hi_bit = (lax.axis_size("lo") * 2**outer_bit).bit_length() - 1
    switched_bits = jnp.concatenate(
        [jnp.array([inner_bit, hi_bit], jnp.int32), level_bits[2:4]]
    )
    coeffs = run_levels(
        coeffs,
        switched_bits,
        [transfers[2], transfers[3], transfers[4], transfers[5]],
        [carried[:, 0], carried[:, 1], carried[:, 2], carried[:, 3]],
    )
    partner = partner_2(coeffs, "lo", inner_bit)
    coeffs = remote_level(coeffs, partner, carried[:, 4], transfers[6], inner_child)
    partner = partner_2(coeffs, "hi", outer_bit)
    coeffs = remote_level(coeffs, partner, carried[:, 5], transfers[7], outer_child)
    coeff_re = coeffs[..., :rank_size]
    coeff_im = coeffs[..., rank_size:]
    stacked = jnp.concatenate(
        [
            jnp.concatenate([coeff_re, -coeff_im], axis=-1),
            jnp.concatenate([coeff_im, coeff_re], axis=-1),
        ],
        axis=1,
    )
    values = jnp.einsum(
        "bmr,bnr->bmn",
        receiver_interp.reshape(blocks_here, LEAF, pair_width),
        stacked,
        preferred_element_type=jnp.float32,
    )
    tree_values = values.astype(jnp.bfloat16).reshape(points, twice_rhs)
    return tree_values[receiver_slot]


def solution(mesh):
    return jax.shard_map(
        per_device,
        mesh=mesh,
        in_specs=(
            P(("hi", "lo"), None),
            P(("hi", "lo")),
            P(("hi", "lo"), None),
            P(("hi", "lo"), None, None),
            P(),
            P(),
            P(("hi", "lo"), None),
            P(("hi", "lo")),
        ),
        out_specs=P(("hi", "lo"), None),
        check_vma=False,
    )
```
